32 devices in a mesh: gx: 4 (over y, core), gy: 8 (over z, x).
Axes of the slice: x: 2, y: 2, z: 4, core: 2. Of those that a mesh axis runs over, the one named last changes fastest.
Arguments:
- hidden_states: bfloat16 [1024, 128], replicated, may hold values from -60 to 60
- item_table: bfloat16 [262144, 128], P(('gx', 'gy')), may hold values from -1.796875 to 1.796875
- targets: int32 [1024], replicated, may hold values from 0 to 262143
Outputs:
- expected: float32 [1024, 128], P(('gx', 'gy'))
- nll: float32 [1024], P(('gx', 'gy'))
The draws below stay inside these ranges and needn't reach their ends.
All inputs are finite; a program needn't handle non-finite values.
Results may differ from the reference program's by a relative error of at most 0.0023.
Values sent between devices are 32-bit elements; how exact they have to be, the bound alone decides.
A program may use at most 64 MiB of HBM per device.

```python
import jax
import jax.numpy as jnp
from jax import lax

D = 128
BLK = 512
P_SIZE = 1024
ITEMS = 262144


def draw_hidden_states(key, part):
    first_key = jax.random.fold_in(jax.random.fold_in(key, 17), 0)
    normal_draw = jax.random.normal(first_key, (P_SIZE, D), jnp.float32)
    result_rows = jnp.clip(normal_draw, -6.0, 6.0)
    return result_rows.astype(jnp.bfloat16)


def plant(entries, own_key, smallest, high):
    longest = entries.shape.index(max(entries.shape))
    spots = []
    for shift in (0, 1):
        where = [jax.random.randint(jax.random.fold_in(own_key, axis), (), 0, length) for axis, length in enumerate(entries.shape)]
        where[longest] = (where[longest] + shift) % entries.shape[longest]
        spots.append(tuple(where))
    return entries.at[spots[0]].set(smallest).at[spots[1]].set(high)


def shard_levels(stream_key, dims, shards, low, largest):
    def one(dim, shards_of):
        draws = jax.random.uniform(jax.random.fold_in(jax.random.fold_in(stream_key, 6), dim), (shards_of,), jnp.float32, low / len(shards), largest / len(shards))
        return jnp.repeat(jnp.exp(draws), dims[dim] // shards_of).reshape((-1,) + (1,) * (len(dims) - dim - 1))

    factor_of = one(*shards[0])
    for cut in shards[1:]:
        factor_of = factor_of * one(*cut)
    return factor_of


def normal_values(rng, dims, spread, limit, pieces=(), dtype=jnp.bfloat16):
    gain = shard_levels(rng, dims, pieces, -0.22, 0.18) if pieces else 1.0
    entries = jax.random.normal(rng, dims, jnp.float32) * spread * gain
    return jnp.minimum(jnp.maximum(entries, -limit), limit).astype(dtype)


def setup_inputs(seed: int = 0) -> dict:
    key_list = jax.random.split(jax.random.key(seed), 4)
    return {
        "hidden_states": draw_hidden_states(jax.random.fold_in(key_list[3], 71), 0),
        "item_table": normal_values(key_list[1], (ITEMS, D), 0.3, 1.796875, ((0, 32),)),
        "targets": plant(jax.random.randint(key_list[2], (P_SIZE,), 0, ITEMS), jax.random.fold_in(key_list[2], 1), 0, ITEMS - 1).astype(jnp.int32),
    }


def reference(hidden_states, item_table, targets):
    nblocks = item_table.shape[0] // BLK
    blocks = item_table.reshape(nblocks, BLK, D)

    def visit_block(carry, block):
        highest, totals, weighted = carry
        scores = lax.dot_general(hidden_states, block, (((1,), (1,)), ((), ())), preferred_element_type=jnp.float32)
        block_max = jnp.max(scores, axis=1)
        exponent = jnp.exp(scores - block_max[:, None])
        block_sum = jnp.sum(exponent, axis=1)
        probs_low = exponent.astype(jnp.bfloat16)
        block_acc = jnp.dot(probs_low, block, preferred_element_type=jnp.float32)
        new_max = jnp.maximum(highest, block_max)
        retain = jnp.exp(highest - new_max)
        rescale = jnp.exp(block_max - new_max)
        totals = totals * retain + block_sum * rescale
        weighted = weighted * retain[:, None] + block_acc * rescale[:, None]
        return (new_max, totals, weighted), None

    start_state = (jnp.full((P_SIZE,), -1e30, jnp.float32), jnp.zeros((P_SIZE,), jnp.float32), jnp.zeros((P_SIZE, D), jnp.float32))
    (highest, totals, weighted), unused_out = lax.scan(visit_block, start_state, blocks)
    target_rows = item_table[targets]
    target_logit = jnp.sum(hidden_states.astype(jnp.float32) * target_rows.astype(jnp.float32), axis=1)
    expected = weighted / totals[:, None]
    nll = highest + jnp.log(totals) - target_logit
    return expected, nll
```

```python
import functools

import jax
import jax.numpy as jnp
from jax import lax
from jax.experimental import pallas as pl
from jax.experimental.pallas import tpu as pltpu
from jax.sharding import PartitionSpec as P

AXES = ("gx", "gy")
BLOCK = 2048
SUB = 256
DEPTH = 512
LEAD = 4
PARTS = 8
CORES = 2
MESH = pl.DeviceIdType.MESH
NT = (((1,), (1,)), ((), ()))


def kernel(ngx, ngy, rows, hid, table, targets, packed,
           hall, hk, tgt, spots, tgt_now, tab, wide, tabt, even, odd, stage, acc, give, take, send, recv,
           give_sem, take_sem, send_sem, recv_sem, load_sem, small_sem):
    positions, width = hid.shape
    items = table.shape[0]
    part = items // PARTS
    lines, side = ngx // CORES, ngy // 2
    half = lines * ngy
    owners = lines * side
    seg = side * rows
    chunk = lines * seg
    stat_row = send.shape[2] - 8
    gx = lax.axis_index("gx")
    gy = lax.axis_index("gy")
    me = gx * ngy + gy
    core, line = lax.rem(gx, CORES), gx // CORES
    zone, spot = gy // side, lax.rem(gy, side)
    place_of_me = line * ngy + gy
    partner = (gx + 1 - 2 * core, gy)

    hid_load = pltpu.make_async_copy(hid, hall, small_sem.at[0])
    hid_load.start()
    loads = []
    for i in range(PARTS):
        at = pl.ds(i * part, part)
        loads.append(pltpu.make_async_copy(table.at[at], tab.at[at], load_sem.at[i]))
        loads[i].start()
    tgt_load = pltpu.make_async_copy(targets, tgt, small_sem.at[1])
    tgt_load.start()

    even[0:8, :] = jnp.zeros((8, chunk), jnp.float32)
    odd[0:8, :] = jnp.zeros((8, chunk), jnp.float32)
    barrier = pltpu.get_barrier_semaphore()

    def greet(k, c):
        other = lax.rem(place_of_me + k, half)
        pl.semaphore_signal(barrier, inc=1, device_id=(other // ngy * CORES + core, lax.rem(other, ngy)),
                            device_id_type=MESH)
        return c

    lax.fori_loop(1, half, greet, 0)
    pl.semaphore_signal(barrier, inc=1, device_id=partner, device_id_type=MESH)

    tabt[width:, :] = jnp.ones((tabt.shape[0] - width, items), jnp.bfloat16)
    wide[items:, :] = jnp.zeros((8, width), jnp.float32)

    def owner_core(k):
        return core if k % 2 else 1 - core

    def owner_zone(k):
        return zone if k >= 2 else 1 - zone

    def start_of(k, y):
        return ((y * CORES + owner_core(k)) * ngy + owner_zone(k) * side) * rows

    def held_of(base):
        b = base // BLOCK
        return (odd if b % 2 else even), base - b * BLOCK

    def score(k, base):
        x = tab[base:base + SUB, :]
        if k == 0:
            wide[base:base + SUB, :] = x.astype(jnp.float32)
        s = lax.dot_general(x, hk[k], NT, preferred_element_type=jnp.float32)
        held, at = held_of(base)
        held[at:at + SUB, :] = s
        return functools.reduce(jnp.maximum, [s[8 * g:8 * g + 8] for g in range(SUB // 8)])

    def top_of(tops):
        return jnp.max(functools.reduce(jnp.maximum, tops), axis=0, keepdims=True)

    def turn(base):
        tabt[0:width, base:base + DEPTH] = tab[base:base + DEPTH, :].T

    def weigh(k, base, new):
        if k == 0:
            turn(base)
        held, at = held_of(base)
        p = jnp.exp(held[at:at + DEPTH, :] - new).astype(jnp.bfloat16)
        return jnp.dot(tabt[:, base:base + DEPTH], p, preferred_element_type=jnp.float32)

    def fetch(k, lo, hi):
        for i in range(lo, hi):
            y, r = i // seg, i % seg
            t = tgt_now[k * lines + y, r]
            stage[i:i + 1, :] = wide[pl.ds(t, 1), :]

    def hits(k):
        return jnp.sum((stage[...] * hk[k].astype(jnp.float32)).T, axis=0, keepdims=True)

    def passing(kk):
        return pltpu.make_async_remote_copy(
            src_ref=give.at[kk], dst_ref=take.at[kk], send_sem=give_sem.at[kk], recv_sem=take_sem.at[kk],
            device_id=partner, device_id_type=MESH)

    def hand_over(kk, highest, hit):
        if kk == 0:
            pl.semaphore_wait(barrier, half)
        give[kk, 0:width, :] = acc[0:width, :]
        give[kk, width:, :] = jnp.concatenate(
            [acc[width:width + 1, :], highest, hit, jnp.zeros((5, chunk), jnp.float32)], axis=0)
        passing(kk).start()

    def send_out(kk, highest, hit):
        passing(kk).wait_recv()
        other = take[kk, width + 1:width + 2, :]
        both = jnp.maximum(highest, other)
        own_share, other_share = jnp.exp(highest - both), jnp.exp(other - both)
        weighted = (acc[0:width, :] * own_share + take[kk, 0:width, :] * other_share).T
        total = acc[width:width + 1, :] * own_share + take[kk, width:width + 1, :] * other_share
        stats = jnp.concatenate(
            [both, total, hit + take[kk, width + 2:width + 3, :], jnp.zeros((5, chunk), jnp.float32)], axis=0)
        for o in range(owners):
            send[kk, o, 0:rows, :] = weighted[o * rows:(o + 1) * rows, :]
            turned = stats if o == 0 else pltpu.roll(stats, chunk - o * rows, 1)
            send[kk, o, stat_row:, :] = turned[:, 0:width]
        for o in range(owners):
            to_line, to_gy = o // side, owner_zone(2 * kk) * side + o % side
            slot = lax.rem(place_of_me - (to_line * ngy + to_gy) - 1 + half, half)
            copy = pltpu.make_async_remote_copy(
                src_ref=send.at[kk, o], dst_ref=recv.at[slot], send_sem=send_sem, recv_sem=recv_sem,
                device_id=(to_line * CORES + core, to_gy), device_id_type=MESH)
            if kk == 0:
                copy.start()
            else:
                pl.when(o != line * side + spot)(copy.start)

    blocks = [(k, b * BLOCK) for k in range(4) for b in range(items // BLOCK)]
    tgt_load.wait()
    for k in range(4):
        for y in range(lines):
            t = tgt[pl.ds(start_of(k, y) // seg, 1), :] - me * items
            spots[k * lines + y:k * lines + y + 1, :] = jnp.where(jnp.logical_and(t >= 0, t < items), t, items)
    hid_load.wait()
    for k in range(4):
        for y in range(lines):
            hk[k, y * seg:(y + 1) * seg, :] = hall[pl.ds(pl.multiple_of(start_of(k, y), seg), seg), :]

    def subs_of(n):
        if n >= len(blocks):
            return []
        k, base = blocks[n]
        return [(k, base + i * SUB) for i in range(BLOCK // SUB)]

    tops = []
    waited = 0
    for k, base in subs_of(0):
        while waited * part < base + SUB:
            loads[waited].wait()
            waited += 1
        tops.append(score(k, base))

    spot_copy = pltpu.make_async_copy(spots, tgt_now, small_sem.at[1])
    spot_copy.start()
    for n, (k, base) in enumerate(blocks):
        top = top_of(tops)
        if n == 1:
            spot_copy.wait()
        first, last = base == 0, base + BLOCK == items
        new = top if first else jnp.maximum(highest, top)
        ahead = subs_of(n + 1)
        tops = []
        if ahead:
            while waited < PARTS and waited * part < ahead[-1][1] + SUB:
                loads[waited].wait()
                waited += 1
        count = BLOCK // DEPTH
        added = None
        for q in range(count + 1):
            upto = len(ahead) if q == count else min(len(ahead), LEAD + len(ahead) * q // count)
            while len(tops) < upto:
                tops.append(score(*ahead[len(tops)]))
            if q < count:
                piece = weigh(k, base + q * DEPTH, new)
                added = piece if added is None else added + piece
                at = base // BLOCK * count + q
                steps = items // DEPTH
                if k == 0:
                    at, steps = at - steps + count, count
                if at >= 0:
                    fetch(k, at * chunk // steps, (at + 1) * chunk // steps)
        acc[...] = added if first else acc[...] * jnp.exp(highest - new) + added
        highest = new
        if last:
            (send_out if k % 2 else hand_over)(k // 2, highest, hits(k))

    for kk in range(2):
        passing(kk).wait_send()
    recv[half - 1] = send[1, line * side + spot]
    most = recv.at[pl.ds(0, half - 1)]
    whole = pltpu.make_async_remote_copy(
        src_ref=most, dst_ref=most, send_sem=send_sem, recv_sem=recv_sem,
        device_id=(gx, gy), device_id_type=MESH)
    whole.wait_send()
    whole.wait_recv()

    tops = recv[:, stat_row, :]
    top = jnp.max(tops, axis=0, keepdims=True)
    factor = jnp.exp(tops - top)
    total = jnp.sum(factor * recv[:, stat_row + 1, :], axis=0, keepdims=True)
    target = jnp.sum(recv[:, stat_row + 2, :], axis=0, keepdims=True)
    packed[stat_row:stat_row + 1, :] = top + jnp.log(total) - target
    share = (factor / total).T
    out = jnp.zeros((rows, width), jnp.float32)
    for s in range(half):
        out = out + share[0:rows, s:s + 1] * recv[s, 0:rows, :]
    packed[0:rows, :] = out


def unpack(rows, stat_row, packed, exp_out, nll_out):
    exp_out[...] = packed[0:rows, :]
    nll_out[...] = packed[stat_row, 0:rows]


def solution(mesh):
    n = mesh.size
    ngx, ngy = mesh.shape["gx"], mesh.shape["gy"]

    def local(hidden_states, item_table, targets):
        positions, width = hidden_states.shape
        items = item_table.shape[0]
        rows = positions // n
        half = n // CORES
        chunk = positions // 4
        seg = chunk // (ngx // CORES)
        tall = -(-rows // 8) * 8 + 8
        vmem = pl.BlockSpec(memory_space=pltpu.VMEM)
        far = pl.BlockSpec(memory_space=pl.ANY)
        packed = pl.pallas_call(
            functools.partial(kernel, ngx, ngy, rows),
            out_shape=pltpu.VMEM((tall, width), jnp.float32),
            in_specs=[far, far, far],
            out_specs=vmem,
            scratch_shapes=[
                pltpu.VMEM((positions, width), jnp.bfloat16),
                pltpu.VMEM((4, chunk, width), jnp.bfloat16),
                pltpu.VMEM((positions // seg, seg), jnp.int32),
                pltpu.VMEM((positions // seg, seg), jnp.int32),
                pltpu.SMEM((positions // seg, seg), jnp.int32),
                pltpu.VMEM((items, width), jnp.bfloat16),
                pltpu.VMEM((items + 8, width), jnp.float32),
                pltpu.VMEM((width + 16, items), jnp.bfloat16),
                pltpu.VMEM((BLOCK, chunk), jnp.float32),
                pltpu.VMEM((BLOCK, chunk), jnp.float32),
                pltpu.VMEM((chunk, width), jnp.float32),
                pltpu.VMEM((width + 16, chunk), jnp.float32),
                pltpu.VMEM((2, width + 8, chunk), jnp.float32),
                pltpu.VMEM((2, width + 8, chunk), jnp.float32),
                pltpu.VMEM((2, half // 2, tall, width), jnp.float32),
                pltpu.VMEM((half, tall, width), jnp.float32),
                pltpu.SemaphoreType.DMA((2,)),
                pltpu.SemaphoreType.DMA((2,)),
                pltpu.SemaphoreType.DMA,
                pltpu.SemaphoreType.DMA,
                pltpu.SemaphoreType.DMA((PARTS,)),
                pltpu.SemaphoreType.DMA((2,)),
            ],
            compiler_params=pltpu.CompilerParams(collective_id=0, has_side_effects=True, vmem_limit_bytes=60000000),
        )(hidden_states, item_table, targets.reshape(positions // seg, seg))
        packed = pltpu.with_memory_space_constraint(packed, pltpu.VMEM)
        return pl.pallas_call(
            functools.partial(unpack, rows, tall - 8),
            out_shape=(jax.ShapeDtypeStruct((rows, width), jnp.float32), jax.ShapeDtypeStruct((rows,), jnp.float32)),
            in_specs=[vmem], out_specs=(vmem, vmem),
        )(packed)

    return jax.shard_map(
        local, mesh=mesh,
        in_specs=(P(), P(AXES, None), P()),
        out_specs=(P(AXES, None), P(AXES)),
        check_vma=False,
    )
```

```python
import functools

import jax
import jax.numpy as jnp
from jax import lax
from jax.experimental import pallas as pl
from jax.experimental.pallas import tpu as pltpu
from jax.sharding import PartitionSpec as P

AXES = ("gx", "gy")
BLOCK = 2048
SUB = 256
DEPTH = 512
LEAD = 3
HOLD = 1
LOG2E = 1.4426950408889634
PARTS = 8
ZONES = 4
MESH = pl.DeviceIdType.MESH
NT = (((1,), (1,)), ((), ()))


def kernel(ngx, ngy, rows, hid, table, targets, packed,
           hall, hk, both, tgt, spots, tgt_now, tab, wide, tabt, even, odd, stage, acc, send, recv, mid, last,
           send_sem, recv_sem, mid_sem, last_sem, load_sem, small_sem):
    positions, width = hid.shape
    items = table.shape[0]
    part = items // PARTS
    side = ngy // ZONES
    members = ngx * side
    seg = side * rows
    chunk = ngx * seg
    stat_row = send.shape[2] - 8
    used = pl.ds(0, stat_row + 3)
    gx = lax.axis_index("gx")
    gy = lax.axis_index("gy")
    me = gx * ngy + gy
    zone, spot = gy // side, lax.rem(gy, side)
    upper = zone // 2
    zones = (3 - 3 * upper, 2 - upper, zone + 1 - 2 * lax.rem(zone, 2), zone)
    shifts = sorted(((a, b) for a in range(ngx) for b in range(side) if a or b), key=lambda ab: (-(ab[0] > 0) - (ab[1] > 0), ab))

    def peer(a, b):
        return (lax.rem(gx + a, ngx), zone * side + lax.rem(spot + b, side))

    def slot_of(a, b):
        return a * side + b - 1

    def twin(k):
        return (gx, zones[k] * side + spot)

    tgt_load = pltpu.make_async_copy(targets, tgt, small_sem.at[1])
    tgt_load.start()
    hid_load = pltpu.make_async_copy(hid, hall, small_sem.at[0])
    hid_load.start()
    loads = []
    for i in range(PARTS):
        at = pl.ds(i * part, part)
        loads.append(pltpu.make_async_copy(table.at[at], tab.at[at], load_sem.at[i]))
        loads[i].start()

    even[0:8, :] = jnp.zeros((8, chunk), jnp.float32)
    odd[0:8, :] = jnp.zeros((8, chunk), jnp.float32)
    barrier = pltpu.get_barrier_semaphore()

    def greet(j, c):
        pl.semaphore_signal(barrier, inc=1, device_id=peer(j // side, lax.rem(j, side)), device_id_type=MESH)
        return c

    lax.fori_loop(1, members, greet, 0)
    for k in range(ZONES - 1):
        pl.semaphore_signal(barrier, inc=1, device_id=twin(k), device_id_type=MESH)

    tabt[width:, :] = jnp.ones((tabt.shape[0] - width, items), jnp.bfloat16)
    wide[items:, :] = jnp.zeros((8, width), jnp.float32)

    def start_of(k, g):
        return (g * ngy + zones[k] * side) * rows

    blocks = []
    for k in range(ZONES):
        sizes = [BLOCK] * (items // BLOCK)
        if k == 0:
            sizes[:1] = [BLOCK // 2]
            sizes.append(BLOCK // 2)
        elif k == ZONES - 1:
            sizes[-1:] = [BLOCK // 2] * 2
        blocks += [(k, sum(sizes[:i]), size) for i, size in enumerate(sizes)]

    def held_of(n):
        return odd if n % 2 else even

    def widen(lo, hi):
        wide[lo:hi, :] = tab[lo:hi, :].astype(jnp.float32)

    early = (blocks[0][2] + blocks[1][2]) // DEPTH
    edges = [blocks[0][2] + (items - blocks[0][2]) // 16 * i // early * 16 for i in range(early + 1)]

    def score(n, at):
        k, base = blocks[n][0], blocks[n][1] + at
        x = tab[base:base + SUB, :]
        if n == 0:
            widen(base, base + SUB)
        s = jnp.dot(jnp.concatenate([x, x], axis=1), both[k], preferred_element_type=jnp.float32)
        held_of(n)[at:at + SUB, :] = s
        return functools.reduce(jnp.maximum, [s[8 * g:8 * g + 8] for g in range(SUB // 8)])

    def top_of(tops):
        return jnp.max(functools.reduce(jnp.maximum, tops), axis=0, keepdims=True)

    def turn(base):
        tabt[0:width, base:base + DEPTH] = tab[base:base + DEPTH, :].T

    def weigh(n, at, new):
        k, base = blocks[n][0], blocks[n][1] + at
        if k == 0:
            turn(base)
        p = jnp.exp2(held_of(n)[at:at + DEPTH, :] - new).astype(jnp.bfloat16)
        return jnp.dot(tabt[:, base:base + DEPTH], p, preferred_element_type=jnp.float32)

    def fetch(k, lo, hi):
        for i in range(lo, hi):
            stage[k % 2, i:i + 1, :] = wide[pl.ds(tgt_now[k * ngx + i // seg, i % seg], 1), :]

    def hits(k):
        return jnp.sum((stage[k % 2] * hk[k].astype(jnp.float32)).T, axis=0, keepdims=True)

    def sending(k, a, b):
        to = lax.rem(gx + a, ngx) * side + lax.rem(spot + b, side)
        return pltpu.make_async_remote_copy(
            src_ref=send.at[k, to, used], dst_ref=(recv.at[k] if k < ZONES - 1 else last).at[slot_of(a, b), used],
            send_sem=send_sem, recv_sem=recv_sem.at[k], device_id=peer(a, b), device_id_type=MESH)

    def crossing(k):
        slot = members - 1 + lax.rem(zone - zones[k] - 1 + ZONES, ZONES)
        return pltpu.make_async_remote_copy(
            src_ref=mid.at[k, used], dst_ref=last.at[slot, used], send_sem=mid_sem, recv_sem=last_sem,
            device_id=twin(k), device_id_type=MESH)

    def send_out(k, highest, hit):
        weighted = acc[0:width, :].T
        stats = jnp.concatenate([highest, acc[width:width + 1, :], hit, jnp.zeros((5, chunk), jnp.float32)], axis=0)
        for m in range(members):
            send[k, m, 0:rows, :] = weighted[m * rows:(m + 1) * rows, :]
            turned = stats if m == 0 else pltpu.roll(stats, chunk - m * rows, 1)
            send[k, m, stat_row:, :] = turned[:, 0:width]
        if k == 0:
            pl.semaphore_wait(barrier, members - 1 + ZONES - 1)
        for a, b in shifts:
            sending(k, a, b).start()

    def merge(parts):
        tops = parts[:, stat_row, :]
        top = jnp.max(tops, axis=0, keepdims=True)
        factor = jnp.exp2(tops - top)
        total = jnp.sum(factor * parts[:, stat_row + 1, :], axis=0, keepdims=True)
        target = jnp.sum(parts[:, stat_row + 2, :], axis=0, keepdims=True)
        return top, total, target, factor

    def gather(parts, share):
        share = share.T
        out = share[0:rows, 0:1] * parts[0, 0:rows, :]
        for s in range(1, parts.shape[0]):
            out = out + share[0:rows, s:s + 1] * parts[s, 0:rows, :]
        return out

    def arrived(k):
        most = (recv.at[k] if k < ZONES - 1 else last).at[pl.ds(0, members - 1), used]
        return pltpu.make_async_remote_copy(
            src_ref=most, dst_ref=most, send_sem=send_sem, recv_sem=recv_sem.at[k],
            device_id=(gx, gy), device_id_type=MESH)

    def relay(k):
        recv[k, members - 1] = send[k, gx * side + spot]
        arrived(k).wait_recv()
        parts = recv.at[k]
        top, total, target, factor = merge(parts)
        mid[k, 0:rows, :] = gather(parts, factor)
        mid[k, stat_row:, :] = jnp.concatenate([top, total, target, jnp.zeros((5, width), jnp.float32)], axis=0)
        crossing(k).start()

    tgt_load.wait()
    for k in range(ZONES):
        for g in range(ngx):
            at = start_of(k, g)
            t = tgt[pl.ds(at // width, 1), :] - me * items
            t = jnp.where(jnp.logical_and(t >= 0, t < items), t, items)
            spots[k * ngx + g:k * ngx + g + 1, :] = pltpu.roll(t, lax.rem(width - lax.rem(at, width), width), 1)
    hid_load.wait()
    def prepare(k):
        parts = []
        for g in range(ngx):
            h = hall[pl.ds(pl.multiple_of(start_of(k, g), seg), seg), :]
            hk[k, g * seg:(g + 1) * seg, :] = h
            scaled = h.astype(jnp.float32) * LOG2E
            high = scaled.astype(jnp.bfloat16)
            parts.append(jnp.concatenate([high, (scaled - high.astype(jnp.float32)).astype(jnp.bfloat16)], axis=1))
        both[k] = jnp.concatenate(parts, axis=0).T

    prepare(0)
    spot_copy = pltpu.make_async_copy(spots, tgt_now, small_sem.at[1])
    spot_copy.start()

    def subs_of(n):
        return [(n, i * SUB) for i in range(blocks[n][2] // SUB)] if n < len(blocks) else []

    tops = []
    drawn = None
    waited = 0
    for n, at in subs_of(0):
        while waited * part < at + SUB:
            loads[waited].wait()
            waited += 1
        tops.append(score(n, at))
    for k in range(1, ZONES):
        prepare(k)
    while waited < PARTS:
        loads[waited].wait()
        waited += 1
    spot_copy.wait()

    due = None
    for n, (k, base, size) in enumerate(blocks):
        top = top_of(tops)
        first, final = base == 0, base + size == items
        new = top if first else jnp.maximum(highest, top)
        if drawn is not None:
            new = jnp.maximum(new, drawn - 3e38)
        ahead = subs_of(n + 1)
        tops = []
        count = size // DEPTH
        added = None
        hold = min(count - 1, HOLD) if due is not None else 0
        for q in range(count + 1):
            upto = len(ahead) if q == count else min(len(ahead), LEAD + len(ahead) * max(0, q - hold) // max(1, count - hold))
            if due is not None and q == hold + 1:
                due()
                due = None
            while len(tops) < upto:
                tops.append(score(*ahead[len(tops)]))
            if q < count:
                piece = weigh(n, q * DEPTH, new)
                added = piece if added is None else added + piece
                if n < 2:
                    i = base // DEPTH + q
                    widen(edges[i], edges[i + 1])
                lo, hi = base + q * DEPTH, base + (q + 1) * DEPTH
                lo, hi = [max(0, v - (blocks[1][1] + blocks[1][2])) if k == 0 else v for v in (lo, hi)]
                whole = items - (blocks[1][1] + blocks[1][2] if k == 0 else 0)
                lo, hi = lo * chunk // whole, hi * chunk // whole
                if hi > lo:
                    fetch(k, lo, hi)
                    got = jnp.max(stage[k % 2, lo:hi, :], axis=0, keepdims=True)
                    drawn = jnp.concatenate([got] * (chunk // width), axis=1)
        acc[...] = added if first else acc[...] * jnp.exp2(highest - new) + added
        highest = new
        if final:
            def due(k=k, highest=highest):
                send_out(k, highest, hits(k))
                if k == 2:
                    relay(0)
    due()

    relay(1)
    relay(2)
    last[members + ZONES - 2] = send[ZONES - 1, gx * side + spot]
    for k in range(ZONES):
        most = send.at[k, pl.ds(0, members - 1), used]
        pltpu.make_async_remote_copy(
            src_ref=most, dst_ref=most, send_sem=send_sem, recv_sem=recv_sem.at[k],
            device_id=(gx, gy), device_id_type=MESH).wait_send()
    crossed = last.at[pl.ds(members - 1, ZONES - 1), used]
    cross = pltpu.make_async_remote_copy(
        src_ref=crossed, dst_ref=crossed, send_sem=mid_sem, recv_sem=last_sem,
        device_id=(gx, gy), device_id_type=MESH)
    cross.wait_send()
    arrived(ZONES - 1).wait_recv()
    cross.wait_recv()
    top, total, target, factor = merge(last)
    packed[stat_row:stat_row + 1, :] = top / LOG2E + jnp.log(total) - target
    packed[0:rows, :] = gather(last, factor / total)


def unpack(rows, stat_row, packed, exp_out, nll_out):
    exp_out[...] = packed[0:rows, :]
    nll_out[...] = packed[stat_row, 0:rows]


def solution(mesh):
    n = mesh.size
    ngx, ngy = mesh.shape["gx"], mesh.shape["gy"]

    def local(hidden_states, item_table, targets):
        positions, width = hidden_states.shape
        items = item_table.shape[0]
        rows = positions // n
        side = ngy // ZONES
        members = ngx * side
        chunk = members * rows
        tall = -(-rows // 8) * 8 + 8
        vmem = pl.BlockSpec(memory_space=pltpu.VMEM)
        far = pl.BlockSpec(memory_space=pl.ANY)
        packed = pl.pallas_call(
            functools.partial(kernel, ngx, ngy, rows),
            out_shape=pltpu.VMEM((tall, width), jnp.float32),
            in_specs=[far, far, far],
            out_specs=vmem,
            scratch_shapes=[
                pltpu.VMEM((positions, width), jnp.bfloat16),
                pltpu.VMEM((ZONES, chunk, width), jnp.bfloat16),
                pltpu.VMEM((ZONES, 2 * width, chunk), jnp.bfloat16),
                pltpu.VMEM((positions // width, width), jnp.int32),
                pltpu.VMEM((ZONES * ngx, width), jnp.int32),
                pltpu.SMEM((ZONES * ngx, width), jnp.int32),
                pltpu.VMEM((items, width), jnp.bfloat16),
                pltpu.VMEM((items + 8, width), jnp.float32),
                pltpu.VMEM((width + 16, items), jnp.bfloat16),
                pltpu.VMEM((BLOCK, chunk), jnp.float32),
                pltpu.VMEM((BLOCK, chunk), jnp.float32),
                pltpu.VMEM((2, chunk, width), jnp.float32),
                pltpu.VMEM((width + 16, chunk), jnp.float32),
                pltpu.VMEM((ZONES, members, tall, width), jnp.float32),
                pltpu.VMEM((ZONES - 1, members, tall, width), jnp.float32),
                pltpu.VMEM((ZONES - 1, tall, width), jnp.float32),
                pltpu.VMEM((members + ZONES - 1, tall, width), jnp.float32),
                pltpu.SemaphoreType.DMA,
                pltpu.SemaphoreType.DMA((ZONES,)),
                pltpu.SemaphoreType.DMA,
                pltpu.SemaphoreType.DMA,
                pltpu.SemaphoreType.DMA((PARTS,)),
                pltpu.SemaphoreType.DMA((2,)),
            ],
            compiler_params=pltpu.CompilerParams(collective_id=0, has_side_effects=True, vmem_limit_bytes=60000000),
        )(hidden_states, item_table, targets.reshape(positions // width, width))
        packed = pltpu.with_memory_space_constraint(packed, pltpu.VMEM)
        return pl.pallas_call(
            functools.partial(unpack, rows, tall - 8),
            out_shape=(jax.ShapeDtypeStruct((rows, width), jnp.float32), jax.ShapeDtypeStruct((rows,), jnp.float32)),
            in_specs=[vmem], out_specs=(vmem, vmem),
        )(packed)

    return jax.shard_map(
        local, mesh=mesh,
        in_specs=(P(), P(AXES, None), P()),
        out_specs=(P(AXES, None), P(AXES)),
        check_vma=False,
    )
```

```python
import functools

import jax
import jax.numpy as jnp
from jax import lax
from jax.experimental import pallas as pl
from jax.experimental.pallas import tpu as pltpu
from jax.sharding import PartitionSpec as P

AXES = ("gx", "gy")
BLOCK = 2048
SUB = 256
DEPTH = 512
LEAD = 3
HOLD = 1
LOG2E = 1.4426950408889634
PARTS = 8
ZONES = 4
MESH = pl.DeviceIdType.MESH
NT = (((1,), (1,)), ((), ()))


def kernel(ngx, ngy, rows, hid, table, targets, packed,
           hall, hk, both, tgt, spots, tgt_now, tab, wide, tabt, even, odd, stage, acc, send, recv, mid, last,
           send_sem, recv_sem, mid_sem, last_sem, load_sem, small_sem):
    positions, width = hid.shape
    items = table.shape[0]
    part = items // PARTS
    side = ngy // ZONES
    members = ngx * side
    seg = side * rows
    chunk = ngx * seg
    stat_row = send.shape[2] - 8
    used = pl.ds(0, stat_row + 3)
    gx = lax.axis_index("gx")
    gy = lax.axis_index("gy")
    me = gx * ngy + gy
    zone, spot = gy // side, lax.rem(gy, side)
    upper = zone // 2
    zones = (3 - 3 * upper, 2 - upper, zone + 1 - 2 * lax.rem(zone, 2), zone)
    shifts = sorted(((a, b) for a in range(ngx) for b in range(side) if a or b), key=lambda ab: (-(ab[0] > 0) - (ab[1] > 0), ab))

    def peer(a, b):
        return (lax.rem(gx + a, ngx), zone * side + lax.rem(spot + b, side))

    def slot_of(a, b):
        return a * side + b - 1

    def twin(k):
        return (gx, zones[k] * side + spot)

    tgt_load = pltpu.make_async_copy(targets, tgt, small_sem.at[1])
    tgt_load.start()
    hid_load = pltpu.make_async_copy(hid, hall, small_sem.at[0])
    hid_load.start()
    loads = []
    for i in range(PARTS):
        at = pl.ds(i * part, part)
        loads.append(pltpu.make_async_copy(table.at[at], tab.at[at], load_sem.at[i]))

    even[0:8, :] = jnp.zeros((8, chunk), jnp.float32)
    odd[0:8, :] = jnp.zeros((8, chunk), jnp.float32)
    barrier = pltpu.get_barrier_semaphore()

    def greet(j, c):
        pl.semaphore_signal(barrier, inc=1, device_id=peer(j // side, lax.rem(j, side)), device_id_type=MESH)
        return c

    lax.fori_loop(1, members, greet, 0)
    for load in loads:
        load.start()
    for k in range(ZONES - 1):
        pl.semaphore_signal(barrier, inc=1, device_id=twin(k), device_id_type=MESH)

    tabt[width:, :] = jnp.ones((tabt.shape[0] - width, items), jnp.bfloat16)
    wide[items:, :] = jnp.zeros((8, width), jnp.float32)

    def start_of(k, g):
        return (g * ngy + zones[k] * side) * rows

    blocks = []
    for k in range(ZONES):
        sizes = [BLOCK] * (items // BLOCK)
        if k == 0:
            sizes[:1] = [BLOCK // 2]
            sizes.append(BLOCK // 2)
        elif k == ZONES - 1:
            sizes[-1:] = [BLOCK // 2] * 2
        blocks += [(k, sum(sizes[:i]), size) for i, size in enumerate(sizes)]

    def held_of(n):
        return odd if n % 2 else even

    def widen(lo, hi):
        wide[lo:hi, :] = tab[lo:hi, :].astype(jnp.float32)

    early = (blocks[0][2] + blocks[1][2]) // DEPTH
    edges = [blocks[0][2] + (items - blocks[0][2]) // 16 * i // early * 16 for i in range(early + 1)]

    def score(n, at):
        k, base = blocks[n][0], blocks[n][1] + at
        x = tab[base:base + SUB, :]
        if n == 0:
            widen(base, base + SUB)
        s = jnp.dot(jnp.concatenate([x, x], axis=1), both[k], preferred_element_type=jnp.float32)
        held_of(n)[at:at + SUB, :] = s
        return functools.reduce(jnp.maximum, [s[8 * g:8 * g + 8] for g in range(SUB // 8)])

    def top_of(tops):
        return jnp.max(functools.reduce(jnp.maximum, tops), axis=0, keepdims=True)

    def turn(base):
        tabt[0:width, base:base + DEPTH] = tab[base:base + DEPTH, :].T

    def weigh(n, at, new):
        k, base = blocks[n][0], blocks[n][1] + at
        if k == 0:
            turn(base)
        p = jnp.exp2(held_of(n)[at:at + DEPTH, :] - new).astype(jnp.bfloat16)
        return jnp.dot(tabt[:, base:base + DEPTH], p, preferred_element_type=jnp.float32)

    def fetch(k, lo, hi):
        for i in range(lo, hi):
            stage[k % 2, i:i + 1, :] = wide[pl.ds(tgt_now[k * ngx + i // seg, i % seg], 1), :]

    def hits(k):
        return jnp.sum((stage[k % 2] * hk[k].astype(jnp.float32)).T, axis=0, keepdims=True)

    def sending(k, a, b):
        to = lax.rem(gx + a, ngx) * side + lax.rem(spot + b, side)
        return pltpu.make_async_remote_copy(
            src_ref=send.at[k, to, used], dst_ref=(recv.at[k] if k < ZONES - 1 else last).at[slot_of(a, b), used],
            send_sem=send_sem, recv_sem=recv_sem.at[k], device_id=peer(a, b), device_id_type=MESH)

    def crossing(k):
        slot = members - 1 + lax.rem(zone - zones[k] - 1 + ZONES, ZONES)
        return pltpu.make_async_remote_copy(
            src_ref=mid.at[k, used], dst_ref=last.at[slot, used], send_sem=mid_sem, recv_sem=last_sem,
            device_id=twin(k), device_id_type=MESH)

    def send_out(k, highest, hit):
        weighted = acc[0:width, :].T
        stats = jnp.concatenate([highest, acc[width:width + 1, :], hit, jnp.zeros((5, chunk), jnp.float32)], axis=0)
        for m in range(members):
            send[k, m, 0:rows, :] = weighted[m * rows:(m + 1) * rows, :]
            turned = stats if m == 0 else pltpu.roll(stats, chunk - m * rows, 1)
            send[k, m, stat_row:, :] = turned[:, 0:width]
        if k == 0:
            pl.semaphore_wait(barrier, members - 1 + ZONES - 1)
        for a, b in shifts:
            sending(k, a, b).start()

    def merge(parts):
        tops = parts[:, stat_row, :]
        top = jnp.max(tops, axis=0, keepdims=True)
        factor = jnp.exp2(tops - top)
        total = jnp.sum(factor * parts[:, stat_row + 1, :], axis=0, keepdims=True)
        target = jnp.sum(parts[:, stat_row + 2, :], axis=0, keepdims=True)
        return top, total, target, factor

    def gather(parts, share):
        share = share.T
        out = share[0:rows, 0:1] * parts[0, 0:rows, :]
        for s in range(1, parts.shape[0]):
            out = out + share[0:rows, s:s + 1] * parts[s, 0:rows, :]
        return out

    def arrived(k):
        most = (recv.at[k] if k < ZONES - 1 else last).at[pl.ds(0, members - 1), used]
        return pltpu.make_async_remote_copy(
            src_ref=most, dst_ref=most, send_sem=send_sem, recv_sem=recv_sem.at[k],
            device_id=(gx, gy), device_id_type=MESH)

    def relay(k):
        recv[k, members - 1] = send[k, gx * side + spot]
        arrived(k).wait_recv()
        parts = recv.at[k]
        top, total, target, factor = merge(parts)
        mid[k, 0:rows, :] = gather(parts, factor)
        mid[k, stat_row:, :] = jnp.concatenate([top, total, target, jnp.zeros((5, width), jnp.float32)], axis=0)
        crossing(k).start()

    tgt_load.wait()
    for k in range(ZONES):
        for g in range(ngx):
            at = start_of(k, g)
            t = tgt[pl.ds(at // width, 1), :] - me * items
            t = jnp.where(jnp.logical_and(t >= 0, t < items), t, items)
            spots[k * ngx + g:k * ngx + g + 1, :] = pltpu.roll(t, lax.rem(width - lax.rem(at, width), width), 1)
    hid_load.wait()
    def prepare(k):
        parts = []
        for g in range(ngx):
            h = hall[pl.ds(pl.multiple_of(start_of(k, g), seg), seg), :]
            hk[k, g * seg:(g + 1) * seg, :] = h
            scaled = h.astype(jnp.float32) * LOG2E
            high = scaled.astype(jnp.bfloat16)
            parts.append(jnp.concatenate([high, (scaled - high.astype(jnp.float32)).astype(jnp.bfloat16)], axis=1))
        both[k] = jnp.concatenate(parts, axis=0).T

    prepare(0)
    spot_copy = pltpu.make_async_copy(spots, tgt_now, small_sem.at[1])
    spot_copy.start()

    def subs_of(n):
        return [(n, i * SUB) for i in range(blocks[n][2] // SUB)] if n < len(blocks) else []

    tops = []
    drawn = None
    waited = 0
    for n, at in subs_of(0):
        while waited * part < at + SUB:
            loads[waited].wait()
            waited += 1
        tops.append(score(n, at))
    for k in range(1, ZONES):
        prepare(k)
    while waited < PARTS:
        loads[waited].wait()
        waited += 1
    spot_copy.wait()

    due = None
    for n, (k, base, size) in enumerate(blocks):
        top = top_of(tops)
        first, final = base == 0, base + size == items
        new = top if first else jnp.maximum(highest, top)
        if drawn is not None:
            new = jnp.maximum(new, drawn - 3e38)
        ahead = subs_of(n + 1)
        tops = []
        count = size // DEPTH
        added = None
        hold = min(count - 1, HOLD) if due is not None else 0
        for q in range(count + 1):
            upto = len(ahead) if q == count else min(len(ahead), LEAD + len(ahead) * max(0, q - hold) // max(1, count - hold))
            if due is not None and q == hold + 1:
                due()
                due = None
            while len(tops) < upto:
                tops.append(score(*ahead[len(tops)]))
            if q < count:
                piece = weigh(n, q * DEPTH, new)
                added = piece if added is None else added + piece
                if n < 2:
                    i = base // DEPTH + q
                    widen(edges[i], edges[i + 1])
                lo, hi = base + q * DEPTH, base + (q + 1) * DEPTH
                lo, hi = [max(0, v - (blocks[1][1] + blocks[1][2])) if k == 0 else v for v in (lo, hi)]
                whole = items - (blocks[1][1] + blocks[1][2] if k == 0 else 0)
                lo, hi = lo * chunk // whole, hi * chunk // whole
                if hi > lo:
                    fetch(k, lo, hi)
                    got = jnp.max(stage[k % 2, lo:hi, :], axis=0, keepdims=True)
                    drawn = jnp.concatenate([got] * (chunk // width), axis=1)
        acc[...] = added if first else acc[...] * jnp.exp2(highest - new) + added
        highest = new
        if final:
            def due(k=k, highest=highest):
                send_out(k, highest, hits(k))
                if k == 2:
                    relay(0)
    due()

    relay(1)
    relay(2)
    last[members + ZONES - 2] = send[ZONES - 1, gx * side + spot]
    for k in range(ZONES):
        most = send.at[k, pl.ds(0, members - 1), used]
        pltpu.make_async_remote_copy(
            src_ref=most, dst_ref=most, send_sem=send_sem, recv_sem=recv_sem.at[k],
            device_id=(gx, gy), device_id_type=MESH).wait_send()
    crossed = last.at[pl.ds(members - 1, ZONES - 1), used]
    cross = pltpu.make_async_remote_copy(
        src_ref=crossed, dst_ref=crossed, send_sem=mid_sem, recv_sem=last_sem,
        device_id=(gx, gy), device_id_type=MESH)
    cross.wait_send()
    arrived(ZONES - 1).wait_recv()
    cross.wait_recv()
    top, total, target, factor = merge(last)
    packed[stat_row:stat_row + 1, :] = top / LOG2E + jnp.log(total) - target
    packed[0:rows, :] = gather(last, factor / total)


def unpack(rows, stat_row, packed, exp_out, nll_out):
    exp_out[...] = packed[0:rows, :]
    nll_out[...] = packed[stat_row, 0:rows]


def solution(mesh):
    n = mesh.size
    ngx, ngy = mesh.shape["gx"], mesh.shape["gy"]

    def local(hidden_states, item_table, targets):
        positions, width = hidden_states.shape
        items = item_table.shape[0]
        rows = positions // n
        side = ngy // ZONES
        members = ngx * side
        chunk = members * rows
        tall = -(-rows // 8) * 8 + 8
        vmem = pl.BlockSpec(memory_space=pltpu.VMEM)
        far = pl.BlockSpec(memory_space=pl.ANY)
        packed = pl.pallas_call(
            functools.partial(kernel, ngx, ngy, rows),
            out_shape=pltpu.VMEM((tall, width), jnp.float32),
            in_specs=[far, far, far],
            out_specs=vmem,
            scratch_shapes=[
                pltpu.VMEM((positions, width), jnp.bfloat16),
                pltpu.VMEM((ZONES, chunk, width), jnp.bfloat16),
                pltpu.VMEM((ZONES, 2 * width, chunk), jnp.bfloat16),
                pltpu.VMEM((positions // width, width), jnp.int32),
                pltpu.VMEM((ZONES * ngx, width), jnp.int32),
                pltpu.SMEM((ZONES * ngx, width), jnp.int32),
                pltpu.VMEM((items, width), jnp.bfloat16),
                pltpu.VMEM((items + 8, width), jnp.float32),
                pltpu.VMEM((width + 16, items), jnp.bfloat16),
                pltpu.VMEM((BLOCK, chunk), jnp.float32),
                pltpu.VMEM((BLOCK, chunk), jnp.float32),
                pltpu.VMEM((2, chunk, width), jnp.float32),
                pltpu.VMEM((width + 16, chunk), jnp.float32),
                pltpu.VMEM((ZONES, members, tall, width), jnp.float32),
                pltpu.VMEM((ZONES - 1, members, tall, width), jnp.float32),
                pltpu.VMEM((ZONES - 1, tall, width), jnp.float32),
                pltpu.VMEM((members + ZONES - 1, tall, width), jnp.float32),
                pltpu.SemaphoreType.DMA,
                pltpu.SemaphoreType.DMA((ZONES,)),
                pltpu.SemaphoreType.DMA,
                pltpu.SemaphoreType.DMA,
                pltpu.SemaphoreType.DMA((PARTS,)),
                pltpu.SemaphoreType.DMA((2,)),
            ],
            compiler_params=pltpu.CompilerParams(collective_id=0, has_side_effects=True, vmem_limit_bytes=60000000),
        )(hidden_states, item_table, targets.reshape(positions // width, width))
        packed = pltpu.with_memory_space_constraint(packed, pltpu.VMEM)
        return pl.pallas_call(
            functools.partial(unpack, rows, tall - 8),
            out_shape=(jax.ShapeDtypeStruct((rows, width), jnp.float32), jax.ShapeDtypeStruct((rows,), jnp.float32)),
            in_specs=[vmem], out_specs=(vmem, vmem),
        )(packed)

    return jax.shard_map(
        local, mesh=mesh,
        in_specs=(P(), P(AXES, None), P()),
        out_specs=(P(AXES, None), P(AXES)),
        check_vma=False,
    )
```
